512 devices in a mesh: row: 16 (over x, y), col: 32 (over z, core).
Axes of the slice: x: 4, y: 4, z: 16, core: 2. Of those that a mesh axis runs over, the one named last changes fastest.
Arguments:
- arrival: float32 [64, 16384], P(None, 'col'), may hold values from 0 to 4
- delay: bfloat16 [4, 16384, 16384], P(None, 'col', 'row'), may hold values from -40 to 20
- occupancy: int32 [4, 32, 32], replicated, may hold values from 0 to 1, as said below
Outputs:
- final_arrival: float32 [64, 16384], P(None, 'col')
- worst: float32 [64], replicated
The draws below stay inside these ranges and needn't reach their ends.
Inputs may be any that keep to these rules, and one draw needn't show every extreme that they name: In every level every column of tiles holds at least one tile with occupancy 1.
All inputs are finite; a program needn't handle non-finite values.
Results may differ from the reference program's by a relative error of at most 0.0009.
Values sent between devices are 32-bit elements; how exact they have to be, the bound alone decides.
No kernel may reach another device: no remote copies, remote signals or barrier semaphores. Data moves between devices by JAX's collectives and lax.ppermute only.
A program may use at most 64 MiB of HBM per device.

```python
import jax
import jax.numpy as jnp
from jax import lax

TILE = 512
SCEN = 64
LEVELS = 4
TILES = 32
PINS = 16384


def draw_occupancy(key, part):
    first, second = jax.random.split(jax.random.fold_in(key, 7))
    base = jax.random.randint(first, (LEVELS, TILES, TILES), 0, 2, dtype=jnp.int32)
    picked = jax.random.randint(second, (LEVELS, 1, TILES), 0, TILES, dtype=jnp.int32)
    places = jnp.arange(TILES, dtype=jnp.int32)[None, :, None]
    forced = (places == picked).astype(jnp.int32)
    return jnp.maximum(base, forced)


def draw_delay(key, part):
    spread = jnp.float32(2.5)
    nominal = spread * jnp.sqrt(2.0 * jnp.log(jnp.float32(0.5 * PINS)))
    first, second, third = jax.random.split(jax.random.fold_in(key, 11), 3)
    normal_part = jnp.clip(jax.random.normal(first, (LEVELS, PINS, PINS), jnp.float32), -6.0, 6.0)
    values = spread * normal_part - nominal
    return jnp.clip(values, -40.0, 20.0).astype(jnp.bfloat16)


def levels(rng, shape, pieces, smallest, high):
    level, own = 1.0, jax.random.fold_in(rng, 6)
    for dim, parts in pieces:
        heights = jnp.exp(jax.random.uniform(jax.random.fold_in(own, dim), (parts,), jnp.float32, smallest / len(pieces), high / len(pieces)))
        level = level * jnp.repeat(heights, shape[dim] // parts).reshape([-1 if axis == dim else 1 for axis in range(len(shape))])
    return level


def setup_inputs(seed: int = 0) -> dict:
    key_list = jax.random.split(jax.random.key(seed), 4)
    return {
        "arrival": jnp.clip(4.0 * jax.random.uniform(key_list[0], (SCEN, PINS), jnp.float32) ** levels(key_list[0], (SCEN, PINS), ((1, 32),), -0.2, 0.2), 0.0, 4.0),
        "delay": draw_delay(jax.random.fold_in(key_list[3], 71), 0),
        "occupancy": draw_occupancy(jax.random.fold_in(key_list[3], 71), 0),
    }


def level_max(times, delay_level, flags):
    width = min(32, TILE)
    turns = PINS // width

    def step(best, index):
        start = (index * width).astype(jnp.int32)
        part_a = lax.dynamic_slice_in_dim(times, start, width, 1)
        part_d = lax.dynamic_slice_in_dim(delay_level, start, width, 0).astype(jnp.float32)
        tile_row = lax.dynamic_index_in_dim(flags, (start // TILE).astype(jnp.int32), 0, keepdims=False)
        keep = jnp.repeat(tile_row > 0, TILE)
        masked = jnp.where(keep[None, :], part_d, jnp.float32(-1e9))
        return jnp.maximum(best, jnp.max(part_a[:, :, None] + masked[None, :, :], axis=1)), None

    init = jnp.full((times.shape[0], PINS), -1e9, jnp.float32)
    best, unused = lax.scan(step, init, jnp.arange(turns, dtype=jnp.int32))
    return best


def reference(arrival, delay, occupancy):
    times = arrival
    for level in range(LEVELS):
        times = level_max(times, delay[level], occupancy[level])
    return times, jnp.max(times, axis=1)
```

```python
import functools

import jax
import jax.numpy as jnp
import numpy as np
from jax import lax
from jax.experimental import pallas as pl
from jax.experimental.pallas import tpu as pltpu
from jax.sharding import Mesh
from jax.sharding import PartitionSpec as P

SUB, LANE = 8, 128
EMPTY = -1000000000.0
CHUNKS = 4
STEP = 8


def level_kernel(level, flags_ref, t_ref, delay_ref, out_ref, raw, wide, sems):
    rows, width = wide.shape
    groups, tiles = t_ref.shape[0], t_ref.shape[1]
    part = rows // CHUNKS
    half = width // 2

    def fetch(chunk):
        span = pl.ds(chunk * part, part)
        return pltpu.make_async_copy(delay_ref.at[level, span, :], raw.at[span, :], sems.at[chunk])

    for chunk in range(CHUNKS):
        fetch(chunk).start()
    out_ref[...] = jnp.full(out_ref.shape, EMPTY, jnp.float32)
    for chunk in range(CHUNKS):
        fetch(chunk).wait()
        span = pl.ds(chunk * part, part)
        for side in range(2):
            cols = slice(side * half, (side + 1) * half)
            value = raw[span, cols].astype(jnp.float32)
            wide[span, cols] = jnp.where(flags_ref[side] > 0, value, jnp.float32(EMPTY))
        tile = chunk
        for block in range(2):
            base = block * (groups // 2)
            n = groups // 2
            lanes = width // LANE

            def step(index, carry):
                held, best = carry
                best = list(best)
                start = chunk * part + index * STEP
                for i in range(STEP):
                    row = jnp.broadcast_to(wide[pl.ds(start + i, 1), :], (SUB, width))
                    for g in range(n):
                        value = jnp.broadcast_to(held[g][:, i : i + 1], (SUB, LANE))
                        for j in range(lanes):
                            k = g * lanes + j
                            best[k] = jnp.maximum(best[k], value + row[:, j * LANE : (j + 1) * LANE])
                held = tuple(pltpu.roll(h, LANE - STEP, 1) for h in held)
                return held, tuple(best)

            held = tuple(t_ref[base + g, tile] for g in range(n))
            place = lambda g, j: (base + g, (j % 4) // 2, j // 4, j % 2)
            best = tuple(out_ref[place(g, j)] for g in range(n) for j in range(lanes))
            held, best = lax.fori_loop(0, part // STEP, step, (held, best))
            for g in range(n):
                for j in range(lanes):
                    out_ref[place(g, j)] = best[g * lanes + j]


def level_max(level, flags, times, delay):
    rows, width = delay.shape[1:]
    groups = times.shape[0]
    work = times.shape[0] * SUB * rows * width
    return pl.pallas_call(
        functools.partial(level_kernel, level),
        out_shape=jax.ShapeDtypeStruct((groups, 2, 2, 2, SUB, LANE), jnp.float32),
        in_specs=[
            pl.BlockSpec(memory_space=pltpu.SMEM),
            pl.BlockSpec(memory_space=pltpu.VMEM),
            pl.BlockSpec(memory_space=pl.ANY),
        ],
        out_specs=pl.BlockSpec(memory_space=pltpu.VMEM),
        scratch_shapes=[
            pltpu.VMEM((rows, width), jnp.bfloat16),
            pltpu.VMEM((rows, width), jnp.float32),
            pltpu.SemaphoreType.DMA((CHUNKS,)),
        ],
        compiler_params=pltpu.CompilerParams(vmem_limit_bytes=16 * 1024 * 1024),
        cost_estimate=pl.CostEstimate(flops=2 * work, bytes_accessed=2 * rows * width, transcendentals=0),
        name="level_max",
    )(flags, times, delay)


def exchange(value, axes):
    return lax.all_to_all(value, axes, split_axis=0, concat_axis=0, tiled=True)


def shards(arrival, delay, occupancy):
    scenarios, pins = arrival.shape
    levels = delay.shape[0]
    plane = lax.axis_size("x") * lax.axis_size("y")
    place = lax.axis_index("x") * lax.axis_size("y") + lax.axis_index("y")
    col = lax.axis_index("z") * lax.axis_size("k") + lax.axis_index("k")
    flags = lax.dynamic_slice(occupancy, (0, col, place * 2), (levels, 1, 2))[:, 0, :]
    groups, tiles = scenarios // SUB, pins // LANE
    times = jnp.transpose(arrival.reshape(groups, SUB, tiles, LANE), (0, 2, 1, 3))
    worst = None
    for level in range(levels):
        last = level == levels - 1
        best = level_max(level, flags[level], times, delay)
        parts = best.reshape(plane * 2, 2, SUB, LANE)
        if last:
            top = jnp.max(best, axis=(1, 2, 3))
            top = jnp.broadcast_to(jnp.max(top, axis=2)[:, :, None], (groups, SUB, LANE))
            top = jnp.max(jnp.where(lax.broadcasted_iota(jnp.int32, (groups, SUB, LANE), 2) == lax.broadcasted_iota(jnp.int32, (groups, SUB, LANE), 0), top, EMPTY), axis=0)
            parts = jnp.concatenate([parts, jnp.broadcast_to(top[None, None], (plane * 2, 1, SUB, LANE))], axis=1)
        got = exchange(parts, ("x", "y", "k"))
        got = got.reshape(plane, 2, *got.shape[1:])
        got = jnp.maximum(got[:, 0], got[:, 1])
        if last:
            top = jnp.max(got[:, 2], axis=0)
            got = jnp.concatenate([got[:, :2], jnp.broadcast_to(top[None, None], (plane, 1, SUB, LANE))], axis=1)
        got = jnp.max(exchange(got, "z"), axis=0)
        if last:
            worst = jnp.transpose(got[2, :, :groups]).reshape(scenarios)
            got = got[:2]
        whole = exchange(jnp.broadcast_to(got[None], (plane, 2, SUB, LANE)), ("x", "y"))
        times = whole.reshape(groups, tiles, SUB, LANE)
    final = jnp.transpose(times, (0, 2, 1, 3)).reshape(scenarios, pins)
    return (final, worst)


def solution(mesh):
    shape = (4, 4, mesh.shape["col"] // 2, 2)
    fine = Mesh(np.asarray(mesh.devices).reshape(shape), ("x", "y", "z", "k"))
    col = ("z", "k")
    placed = (P(None, col), P(None, col, ("x", "y")), P())
    return jax.shard_map(
        shards, mesh=fine, in_specs=placed, out_specs=(P(None, col), P()), check_vma=False
    )
```

```python
import functools

import jax
import jax.numpy as jnp
import numpy as np
from jax import lax
from jax.experimental import pallas as pl
from jax.experimental.pallas import tpu as pltpu
from jax.sharding import Mesh
from jax.sharding import PartitionSpec as P

SUB, LANE = 8, 128
EMPTY = -1000000000.0
GROUPS = 8
LANES = 8
SHIFT = 8
TURNS = 4


def level_body(flags_ref, t_ref, delay_ref, out_ref, spread_a, spread_b, wide, turned):
    tiles = t_ref.shape[1]
    rotations = LANE // (SHIFT * TURNS)
    chunk = tiles * SHIFT

    for m in range(rotations):
        for tile in range(tiles):
            for g in range(GROUPS):
                value = t_ref[g, tile]
                turned[m, tile, g] = pltpu.roll(value, LANE - m * SHIFT * TURNS, 1) if m else value
    out_ref[...] = jnp.full(out_ref.shape, EMPTY, jnp.float32)

    def spread_one(dest, m, e, q, a, g, held):
        lane = e * SHIFT + a
        dest[q * SHIFT + a, g] = jnp.broadcast_to(held[g][:, lane : lane + 1], (SUB, LANE))

    def warm(q, _):
        held = [turned[0, q, g] for g in range(GROUPS)]
        for a in range(SHIFT):
            for g in range(GROUPS):
                spread_one(spread_a, 0, 0, q, a, g, held)
        rows = pl.ds(pl.multiple_of(q * LANE, LANE), LANE)
        for j in range(LANES):
            value = delay_ref[rows, j * LANE : (j + 1) * LANE].astype(jnp.float32)
            wide[j, rows, :] = jnp.where(flags_ref[j // 4] > 0, value, jnp.float32(EMPTY))
        return 0

    lax.fori_loop(0, tiles, warm, 0)

    def stage(m, e, source, dest):
        next_m = m if e + 1 < TURNS else jnp.minimum(m + 1, rotations - 1)
        next_e = (e + 1) % TURNS

        def body(q, _):
            gb = (q // 2) * 4
            side = q % 2
            held = [turned[next_m, q, g] for g in range(GROUPS)]
            keys = [(g, j) for g in range(4) for j in range(4)]
            best = {(g, j): out_ref[gb + g, j // 2, side, j % 2] for g, j in keys}
            todo = [(a, g) for a in range(SHIFT) for g in range(GROUPS)]
            for k in range(chunk):
                place = (k // SHIFT) * LANE + e * SHIFT + k % SHIFT
                at = pl.ds(m * (SHIFT * TURNS) + place, 1)
                row = [jnp.broadcast_to(wide[side * 4 + j, at, :], (SUB, LANE)) for j in range(4)]
                for g in range(4):
                    value = source[k, gb + g]
                    for j in range(4):
                        best[g, j] = jnp.maximum(best[g, j], value + row[j])
                for _ in range(2):
                    a, g = todo.pop(0)
                    spread_one(dest, next_m, next_e, q, a, g, held)
            for g, j in keys:
                out_ref[gb + g, j // 2, side, j % 2] = best[g, j]
            return 0

        lax.fori_loop(0, 4, body, 0)

    def rotation(m, _):
        for e in range(TURNS):
            pair = (spread_a, spread_b) if e % 2 == 0 else (spread_b, spread_a)
            stage(m, e, *pair)
        return 0

    lax.fori_loop(0, rotations, rotation, 0)


def first_kernel(flags_ref, t_ref, delay_ref, out_ref, later_ref, spread_a, spread_b, wide, turned, raw, sems):
    own = pltpu.make_async_copy(delay_ref.at[0], raw, sems.at[0])
    own.start()
    rest = pltpu.make_async_copy(delay_ref.at[pl.ds(1, later_ref.shape[0])], later_ref, sems.at[1])
    rest.start()
    own.wait()
    level_body(flags_ref, t_ref, raw, out_ref, spread_a, spread_b, wide, turned)
    rest.wait()


def later_kernel(level, flags_ref, t_ref, later_ref, out_ref, spread_a, spread_b, wide, turned):
    level_body(flags_ref, t_ref, later_ref.at[level - 1], out_ref, spread_a, spread_b, wide, turned)


def level_max(level, flags, times, delay):
    rows, width = delay.shape[1:]
    tiles = rows // LANE
    work = GROUPS * SUB * rows * width
    vmem = pl.BlockSpec(memory_space=pltpu.VMEM)
    shape = jax.ShapeDtypeStruct((GROUPS, 2, 2, 2, SUB, LANE), jnp.float32)
    scratch = [
        pltpu.VMEM((tiles * SHIFT, GROUPS, SUB, LANE), jnp.float32),
        pltpu.VMEM((tiles * SHIFT, GROUPS, SUB, LANE), jnp.float32),
        pltpu.VMEM((LANES, rows, LANE), jnp.float32),
        pltpu.VMEM((LANE // (SHIFT * TURNS), tiles, GROUPS, SUB, LANE), jnp.float32),
    ]
    common = dict(
        compiler_params=pltpu.CompilerParams(vmem_limit_bytes=16 * 1024 * 1024),
        cost_estimate=pl.CostEstimate(flops=2 * work, bytes_accessed=2 * rows * width, transcendentals=0),
    )
    smem = pl.BlockSpec(memory_space=pltpu.SMEM)
    if level == 0:
        rest = jax.ShapeDtypeStruct((delay.shape[0] - 1, rows, width), delay.dtype)
        return pl.pallas_call(
            first_kernel,
            out_shape=(shape, rest),
            in_specs=[smem, vmem, pl.BlockSpec(memory_space=pltpu.HBM)],
            out_specs=(vmem, vmem),
            scratch_shapes=scratch + [pltpu.VMEM((rows, width), delay.dtype), pltpu.SemaphoreType.DMA((2,))],
            name="first_level",
            **common,
        )(flags, times, delay)
    return pl.pallas_call(
        functools.partial(later_kernel, level),
        out_shape=shape,
        in_specs=[smem, vmem, vmem],
        out_specs=vmem,
        scratch_shapes=scratch,
        name="later_level",
        **common,
    )(flags, times, delay)


def exchange(value, axes):
    return lax.all_to_all(value, axes, split_axis=0, concat_axis=0, tiled=True)


def shards(arrival, delay, occupancy):
    scenarios, pins = arrival.shape
    levels = delay.shape[0]
    plane = lax.axis_size("x") * lax.axis_size("y")
    place = lax.axis_index("x") * lax.axis_size("y") + lax.axis_index("y")
    col = lax.axis_index("z") * lax.axis_size("k") + lax.axis_index("k")
    flags = lax.dynamic_slice(occupancy, (0, col, place * 2), (levels, 1, 2))[:, 0, :]
    groups, tiles = scenarios // SUB, pins // LANE
    times = jnp.transpose(arrival.reshape(groups, SUB, tiles, LANE), (0, 2, 1, 3))
    worst = None
    for level in range(levels):
        last = level == levels - 1
        if level == 0:
            best, later = level_max(level, flags[level], times, delay)
        else:
            best = level_max(level, flags[level], times, later)
        parts = best.reshape(plane * 2, 2, SUB, LANE)
        if last:
            top = jnp.max(best, axis=(1, 2, 3))
            top = jnp.broadcast_to(jnp.max(top, axis=2)[:, :, None], (groups, SUB, LANE))
            top = jnp.max(jnp.where(lax.broadcasted_iota(jnp.int32, (groups, SUB, LANE), 2) == lax.broadcasted_iota(jnp.int32, (groups, SUB, LANE), 0), top, EMPTY), axis=0)
            parts = jnp.concatenate([parts, jnp.broadcast_to(top[None, None], (plane * 2, 1, SUB, LANE))], axis=1)
        got = exchange(parts, ("x", "y", "k"))
        got = got.reshape(plane, 2, *got.shape[1:])
        got = jnp.maximum(got[:, 0], got[:, 1])
        if last:
            top = jnp.max(got[:, 2], axis=0)
            got = jnp.concatenate([got[:, :2], jnp.broadcast_to(top[None, None], (plane, 1, SUB, LANE))], axis=1)
        got = jnp.max(exchange(got, "z"), axis=0)
        if last:
            worst = jnp.transpose(got[2, :, :groups]).reshape(scenarios)
            got = got[:2]
        whole = exchange(jnp.broadcast_to(got[None], (plane, 2, SUB, LANE)), ("x", "y"))
        times = whole.reshape(groups, tiles, SUB, LANE)
    final = jnp.transpose(times, (0, 2, 1, 3)).reshape(scenarios, pins)
    return (final, worst)


def solution(mesh):
    shape = (4, 4, mesh.shape["col"] // 2, 2)
    fine = Mesh(np.asarray(mesh.devices).reshape(shape), ("x", "y", "z", "k"))
    col = ("z", "k")
    placed = (P(None, col), P(None, col, ("x", "y")), P())
    return jax.shard_map(
        shards, mesh=fine, in_specs=placed, out_specs=(P(None, col), P()), check_vma=False
    )
```

```python
import functools

import jax
import jax.numpy as jnp
import numpy as np
from jax import lax
from jax.experimental import pallas as pl
from jax.experimental.pallas import tpu as pltpu
from jax.sharding import Mesh
from jax.sharding import PartitionSpec as P

SUB, LANE = 8, 128
EMPTY = -1000000000.0
HALF = 4
TILES = 4
SHIFT = 8
TURNS = 4


def half_body(times, convert, wide, out_ref, spread_a, spread_b, turned):
    rotations = LANE // (SHIFT * TURNS)
    chunk = TILES * SHIFT

    for m in range(rotations):
        for tile in range(TILES):
            for g in range(HALF):
                value = times(g, tile)
                turned[m, tile, g] = pltpu.roll(value, LANE - m * SHIFT * TURNS, 1) if m else value
    out_ref[...] = jnp.full(out_ref.shape, EMPTY, jnp.float32)

    def held_rows(m, q):
        return {(t, g): turned[m, q * 2 + t, g] for t in range(2) for g in range(HALF)}

    def spread_one(dest, e, q, place, held):
        a, t, g = place
        lane = e * SHIFT + a
        row = (q * 2 + t) * SHIFT + a
        dest[row, g] = jnp.broadcast_to(held[t, g][:, lane : lane + 1], (SUB, LANE))

    places = [(a, t, g) for a in range(SHIFT) for t in range(2) for g in range(HALF)]

    def warm(q, _):
        held = held_rows(0, q)
        for place in places:
            spread_one(spread_a, 0, q, place, held)
        convert(q)
        return 0

    lax.fori_loop(0, 2, warm, 0)

    def stage(m, e, source, dest):
        next_m = m if e + 1 < TURNS else jnp.minimum(m + 1, rotations - 1)
        next_e = (e + 1) % TURNS

        def body(side, _):
            held = held_rows(next_m, side)
            keys = [(g, j) for g in range(HALF) for j in range(4)]
            best = {(g, j): out_ref[g, j, side] for g, j in keys}
            todo = list(places)
            for k in range(chunk):
                place = (k // SHIFT) * LANE + e * SHIFT + k % SHIFT
                at = pl.ds(m * (SHIFT * TURNS) + place, 1)
                row = [jnp.broadcast_to(wide[side * 4 + j, at, :], (SUB, LANE)) for j in range(4)]
                for g in range(HALF):
                    value = source[k, g]
                    for j in range(4):
                        best[g, j] = jnp.maximum(best[g, j], value + row[j])
                for _ in range(2):
                    spread_one(dest, next_e, side, todo.pop(0), held)
            for g, j in keys:
                out_ref[g, j, side] = best[g, j]
            return 0

        lax.fori_loop(0, 2, body, 0)

    def rotation(m, _):
        for e in range(TURNS):
            pair = (spread_a, spread_b) if e % 2 == 0 else (spread_b, spread_a)
            stage(m, e, *pair)
        return 0

    lax.fori_loop(0, rotations, rotation, 0)


def times_of(t_ref, half):
    if len(t_ref.shape) == 4:
        return lambda g, tile: t_ref[half * HALF + g, tile]
    return lambda g, tile: t_ref[g, tile, half]


def sent_kernel(level, flags_ref, t_ref, delay_ref, out_ref, wide, *scratch):
    def convert(q):
        rows = pl.ds(pl.multiple_of(q * 2 * LANE, LANE), 2 * LANE)
        for j in range(8):
            value = delay_ref[level, rows, j * LANE : (j + 1) * LANE].astype(jnp.float32)
            wide[j, rows, :] = jnp.where(flags_ref[j // 4] > 0, value, jnp.float32(EMPTY))

    half_body(times_of(t_ref, flags_ref[2]), convert, wide, out_ref, *scratch)


def kept_kernel(flags_ref, t_ref, wide, out_ref, *scratch):
    half_body(times_of(t_ref, flags_ref[3]), lambda q: None, wide, out_ref, *scratch)


def half_max(level, flags, times, source, shape):
    levels, rows, width = shape
    work = HALF * SUB * rows * width
    vmem = pl.BlockSpec(memory_space=pltpu.VMEM)
    out = jax.ShapeDtypeStruct((HALF, 4, 2, SUB, LANE), jnp.float32)
    wide = jax.ShapeDtypeStruct((width // LANE, rows, LANE), jnp.float32)
    spread = pltpu.VMEM((TILES * SHIFT, HALF, SUB, LANE), jnp.float32)
    sent = level is not None
    return pl.pallas_call(
        functools.partial(sent_kernel, level) if sent else kept_kernel,
        out_shape=(out, wide) if sent else out,
        in_specs=[pl.BlockSpec(memory_space=pltpu.SMEM), vmem, vmem],
        out_specs=(vmem, vmem) if sent else vmem,
        scratch_shapes=[
            spread,
            spread,
            pltpu.VMEM((LANE // (SHIFT * TURNS), TILES, HALF, SUB, LANE), jnp.float32),
        ],
        compiler_params=pltpu.CompilerParams(vmem_limit_bytes=16 * 1024 * 1024),
        cost_estimate=pl.CostEstimate(flops=2 * work, bytes_accessed=2 * rows * width, transcendentals=0),
        name="sent_half" if sent else "kept_half",
    )(flags, times, source)


def exchange(value, axes):
    return lax.all_to_all(value, axes, split_axis=0, concat_axis=0, tiled=True)


def shards(arrival, delay, occupancy):
    scenarios, pins = arrival.shape
    levels = delay.shape[0]
    plane = lax.axis_size("x") * lax.axis_size("y")
    depth = lax.axis_size("z")
    place = lax.axis_index("x") * lax.axis_size("y") + lax.axis_index("y")
    odd = lax.axis_index("z") % 2
    col = lax.axis_index("z") * lax.axis_size("k") + lax.axis_index("k")
    flags = lax.dynamic_slice(occupancy, (0, col, place * 2), (levels, 1, 2))[:, 0, :]
    halves = jnp.broadcast_to(jnp.stack([1 - odd, odd])[None], (levels, 2))
    flags = jnp.concatenate([flags, halves], axis=1)
    groups, tiles = scenarios // SUB, pins // LANE
    neighbour = [(z, z ^ 1) for z in range(depth)]
    times = jnp.transpose(arrival.reshape(groups, SUB, tiles, LANE), (0, 2, 1, 3))
    worst = None
    for level in range(levels):
        last = level == levels - 1
        sent, wide = half_max(0 if level == 0 else level, flags[level], times, delay[:1] if level == 0 else delay, delay.shape)
        got = lax.ppermute(sent, "z", neighbour)
        kept = half_max(None, flags[level], times, wide, delay.shape)
        best = jnp.maximum(kept, got)
        parts = best.reshape(plane * 2, 1, SUB, LANE)
        if last:
            top = jnp.max(jnp.max(best, axis=(1, 2)), axis=2)
            spot = lax.broadcasted_iota(jnp.int32, (HALF, SUB, LANE), 0) + odd * HALF
            here = lax.broadcasted_iota(jnp.int32, (HALF, SUB, LANE), 2) == spot
            top = jnp.max(jnp.where(here, top[:, :, None], EMPTY), axis=0)
            parts = jnp.concatenate([parts, jnp.broadcast_to(top[None, None], parts.shape)], axis=1)
        got = exchange(parts, ("x", "y", "k"))
        got = got.reshape(plane, 2, *got.shape[1:])
        got = jnp.maximum(got[:, 0], got[:, 1])
        if last:
            top = jnp.max(got[:, 1], axis=0)
            got = jnp.concatenate([got[:, :1], jnp.broadcast_to(top[None, None], (plane, 1, SUB, LANE))], axis=1)
        got = exchange(got, "z")
        if last:
            worst = jnp.transpose(jnp.max(got[:, 1], axis=0)[:, :groups]).reshape(scenarios)
        got = jnp.max(got[:, 0].reshape(depth // 2, 2, SUB, LANE), axis=0)
        whole = exchange(jnp.broadcast_to(got[None], (plane, 2, SUB, LANE)), ("x", "y"))
        times = whole.reshape(HALF, tiles, 2, SUB, LANE)
    final = jnp.transpose(times, (2, 0, 3, 1, 4)).reshape(scenarios, pins)
    return (final, worst)


def solution(mesh):
    shape = (4, 4, mesh.shape["col"] // 2, 2)
    fine = Mesh(np.asarray(mesh.devices).reshape(shape), ("x", "y", "z", "k"))
    col = ("z", "k")
    placed = (P(None, col), P(None, col, ("x", "y")), P())
    return jax.shard_map(
        shards, mesh=fine, in_specs=placed, out_specs=(P(None, col), P()), check_vma=False
    )
```

```python
import functools

import jax
import jax.numpy as jnp
import numpy as np
from jax import lax
from jax.experimental import pallas as pl
from jax.experimental.pallas import tpu as pltpu
from jax.sharding import Mesh
from jax.sharding import PartitionSpec as P

SUB, LANE = 8, 128
EMPTY = -1000000000.0
HALF = 4
TILES = 4
SHIFT = 8
TURNS = 4


def half_body(times, convert, wide, out_ref, spread_a, spread_b, turned):
    rotations = LANE // (SHIFT * TURNS)
    chunk = TILES * SHIFT

    for m in range(rotations):
        for tile in range(TILES):
            for g in range(HALF):
                value = times(g, tile)
                turned[m, tile, g] = pltpu.roll(value, LANE - m * SHIFT * TURNS, 1) if m else value
    out_ref[...] = jnp.full(out_ref.shape, EMPTY, jnp.float32)

    def held_rows(m, q):
        return {(t, g): turned[m, q * 2 + t, g] for t in range(2) for g in range(HALF)}

    def spread_one(dest, e, q, place, held):
        a, t, g = place
        lane = e * SHIFT + a
        row = (q * 2 + t) * SHIFT + a
        dest[row, g] = jnp.broadcast_to(held[t, g][:, lane : lane + 1], (SUB, LANE))

    places = [(a, t, g) for a in range(SHIFT) for t in range(2) for g in range(HALF)]

    def warm(q, _):
        held = held_rows(0, q)
        for place in places:
            spread_one(spread_a, 0, q, place, held)
        convert(q)
        return 0

    for q in range(2):
        warm(q, 0)

    def stage(m, e, source, dest):
        next_m = m if e + 1 < TURNS else jnp.minimum(m + 1, rotations - 1)
        next_e = (e + 1) % TURNS

        def body(q, _):
            side = lax.rem(q, 2)
            late = (q // 2) * HALF
            held = held_rows(next_m, q)
            keys = [(g, j) for g in range(HALF) for j in range(4)]
            best = {(g, j): out_ref[g, j, side] for g, j in keys}
            todo = list(places)
            for k in range(chunk):
                place = (k // SHIFT) * LANE + e * SHIFT + k % SHIFT
                at = pl.ds(m * (SHIFT * TURNS) + place, 1)
                row = [jnp.broadcast_to(wide[side * 4 + j, at, :], (SUB, LANE)) for j in range(4)]
                for g in range(HALF):
                    value = source[k, late + g]
                    for j in range(4):
                        best[g, j] = jnp.maximum(best[g, j], value + row[j])
                for _ in range(2):
                    spread_one(dest, next_e, q, todo.pop(0), held)
            for g, j in keys:
                out_ref[g, j, side] = best[g, j]
            return 0

        lax.fori_loop(0, 2, body, 0)

    def rotation(m, _):
        for e in range(TURNS):
            pair = (spread_a, spread_b) if e % 2 == 0 else (spread_b, spread_a)
            stage(m, e, *pair)
        return 0

    lax.fori_loop(0, rotations, rotation, 0)


def times_of(t_ref, half):
    if len(t_ref.shape) == 4:
        return lambda g, tile: t_ref[half * HALF + g, tile]
    return lambda g, tile: t_ref[g, tile, half]


def sent_kernel(level, flags_ref, t_ref, delay_ref, out_ref, wide, *scratch):
    def convert(q):
        rows = pl.ds(q * 2 * LANE, 2 * LANE)
        for j in range(8):
            value = delay_ref[level, rows, j * LANE : (j + 1) * LANE].astype(jnp.float32)
            wide[j, rows, :] = jnp.where(flags_ref[j // 4] > 0, value, jnp.float32(EMPTY))

    half_body(times_of(t_ref, flags_ref[2]), convert, wide, out_ref, *scratch)


def kept_kernel(flags_ref, t_ref, wide, out_ref, *scratch):
    half_body(times_of(t_ref, flags_ref[3]), lambda q: None, wide, out_ref, *scratch)


def half_max(level, flags, times, source, shape):
    levels, rows, width = shape
    work = HALF * SUB * rows * width
    vmem = pl.BlockSpec(memory_space=pltpu.VMEM)
    out = jax.ShapeDtypeStruct((HALF, 4, 2, SUB, LANE), jnp.float32)
    wide = jax.ShapeDtypeStruct((width // LANE, rows, LANE), jnp.float32)
    spread = pltpu.VMEM((TILES * SHIFT, HALF, SUB, LANE), jnp.float32)
    sent = level is not None
    return pl.pallas_call(
        functools.partial(sent_kernel, level) if sent else kept_kernel,
        out_shape=(out, wide) if sent else out,
        in_specs=[pl.BlockSpec(memory_space=pltpu.SMEM), vmem, vmem],
        out_specs=(vmem, vmem) if sent else vmem,
        scratch_shapes=[
            spread,
            spread,
            pltpu.VMEM((LANE // (SHIFT * TURNS), TILES, HALF, SUB, LANE), jnp.float32),
        ],
        compiler_params=pltpu.CompilerParams(vmem_limit_bytes=16 * 1024 * 1024),
        cost_estimate=pl.CostEstimate(flops=2 * work, bytes_accessed=2 * rows * width, transcendentals=0),
        name="sent_half" if sent else "kept_half",
    )(flags, times, source)


def exchange(value, axes):
    return lax.all_to_all(value, axes, split_axis=0, concat_axis=0, tiled=True)


def shards(arrival, delay, occupancy):
    scenarios, pins = arrival.shape
    levels = delay.shape[0]
    plane = lax.axis_size("x") * lax.axis_size("y")
    depth = lax.axis_size("z")
    place = lax.axis_index("x") * lax.axis_size("y") + lax.axis_index("y")
    odd = lax.axis_index("z") % 2
    col = lax.axis_index("z") * lax.axis_size("k") + lax.axis_index("k")
    flags = lax.dynamic_slice(occupancy, (0, col, place * 2), (levels, 1, 2))[:, 0, :]
    halves = jnp.broadcast_to(jnp.stack([1 - odd, odd])[None], (levels, 2))
    flags = jnp.concatenate([flags, halves], axis=1)
    groups, tiles = scenarios // SUB, pins // LANE
    neighbour = [(z, z ^ 1) for z in range(depth)]
    times = jnp.transpose(arrival.reshape(groups, SUB, tiles, LANE), (0, 2, 1, 3))
    worst = None
    for level in range(levels):
        last = level == levels - 1
        sent, wide = half_max(0 if level == 0 else level, flags[level], times, delay[:1] if level == 0 else delay, delay.shape)
        got = lax.ppermute(sent, "z", neighbour)
        kept = half_max(None, flags[level], times, wide, delay.shape)
        best = jnp.maximum(kept, got)
        parts = best.reshape(plane * 2, 1, SUB, LANE)
        if last:
            top = jnp.max(jnp.max(best, axis=(1, 2)), axis=2)
            spot = lax.broadcasted_iota(jnp.int32, (HALF, SUB, LANE), 0) + odd * HALF
            here = lax.broadcasted_iota(jnp.int32, (HALF, SUB, LANE), 2) == spot
            top = jnp.max(jnp.where(here, top[:, :, None], EMPTY), axis=0)
            parts = jnp.concatenate([parts, jnp.broadcast_to(top[None, None], parts.shape)], axis=1)
        got = exchange(parts, ("x", "y", "k"))
        got = got.reshape(plane, 2, *got.shape[1:])
        got = jnp.maximum(got[:, 0], got[:, 1])
        if last:
            top = jnp.max(got[:, 1], axis=0)
            got = jnp.concatenate([got[:, :1], jnp.broadcast_to(top[None, None], (plane, 1, SUB, LANE))], axis=1)
        got = exchange(got, "z")
        if last:
            worst = jnp.transpose(jnp.max(got[:, 1], axis=0)[:, :groups]).reshape(scenarios)
        got = jnp.max(got[:, 0].reshape(depth // 2, 2, SUB, LANE), axis=0)
        whole = exchange(jnp.broadcast_to(got[None], (plane, 2, SUB, LANE)), ("x", "y"))
        times = whole.reshape(HALF, tiles, 2, SUB, LANE)
    final = jnp.transpose(times, (2, 0, 3, 1, 4)).reshape(scenarios, pins)
    return (final, worst)


def solution(mesh):
    shape = (4, 4, mesh.shape["col"] // 2, 2)
    fine = Mesh(np.asarray(mesh.devices).reshape(shape), ("x", "y", "z", "k"))
    col = ("z", "k")
    placed = (P(None, col), P(None, col, ("x", "y")), P())
    return jax.shard_map(
        shards, mesh=fine, in_specs=placed, out_specs=(P(None, col), P()), check_vma=False
    )
```

```python
import functools

import jax
import jax.numpy as jnp
import numpy as np
from jax import lax
from jax.experimental import pallas as pl
from jax.experimental.pallas import tpu as pltpu
from jax.sharding import Mesh
from jax.sharding import PartitionSpec as P

SUB, LANE = 8, 128
EMPTY = -1000000000.0
BOUND = 1000000000.0
HALF = 4
TILES = 4
SHIFT = 8
TURNS = 4


def half_body(times, convert, wide, out_ref, spread_a, spread_b, turned):
    rotations = LANE // (SHIFT * TURNS)
    chunk = TILES * SHIFT

    for m in range(rotations):
        for tile in range(TILES):
            for g in range(HALF):
                value = times(g, tile)
                turned[m, tile, g] = pltpu.roll(value, LANE - m * SHIFT * TURNS, 1) if m else value
    out_ref[...] = jnp.full(out_ref.shape, EMPTY, jnp.float32)

    def held_rows(m, q):
        return {(t, g): turned[m, q * 2 + t, g] for t in range(2) for g in range(HALF)}

    def spread_one(dest, e, q, place, held):
        a, t, g = place
        lane = e * SHIFT + a
        row = (q * 2 + t) * SHIFT + a
        dest[row, g] = jnp.broadcast_to(held[t, g][:, lane : lane + 1], (SUB, LANE))

    places = [(a, t, g) for a in range(SHIFT) for t in range(2) for g in range(HALF)]

    def warm(q, _):
        held = held_rows(0, q)
        for place in places:
            spread_one(spread_a, 0, q, place, held)
        convert(q)
        return 0

    for q in range(2):
        warm(q, 0)

    def stage(m, e, source, dest):
        next_m = m if e + 1 < TURNS else jnp.minimum(m + 1, rotations - 1)
        next_e = (e + 1) % TURNS

        def body(q, _):
            side = lax.rem(q, 2)
            late = (q // 2) * HALF
            held = held_rows(next_m, q)
            keys = [(g, j) for g in range(HALF) for j in range(4)]
            best = {(g, j): out_ref[g, j, side] for g, j in keys}
            todo = list(places)
            for k in range(chunk):
                place = (k // SHIFT) * LANE + e * SHIFT + k % SHIFT
                at = pl.ds(m * (SHIFT * TURNS) + place, 1)
                row = [jnp.broadcast_to(wide[side * 4 + j, at, :], (SUB, LANE)) for j in range(4)]
                for g in range(HALF):
                    value = source[k, late + g]
                    for j in range(4):
                        best[g, j] = jnp.maximum(best[g, j], value + row[j])
                for _ in range(2):
                    spread_one(dest, next_e, q, todo.pop(0), held)
            for g, j in keys:
                out_ref[g, j, side] = best[g, j]
            return 0

        lax.fori_loop(0, 2, body, 0)

    def rotation(m, _):
        for e in range(TURNS):
            pair = (spread_a, spread_b) if e % 2 == 0 else (spread_b, spread_a)
            stage(m, e, *pair)
        return 0

    lax.fori_loop(0, rotations, rotation, 0)


def times_of(t_ref, half):
    if len(t_ref.shape) == 4:
        return lambda g, tile: t_ref[half * HALF + g, tile]
    return lambda g, tile: t_ref[g, tile, half]


def parity():
    return lax.rem(lax.axis_index("z"), 2)


def sent_kernel(level, caps_ref, t_ref, delay_ref, out_ref, wide, *scratch):
    slab = level if delay_ref.shape[0] > 1 else 0

    def convert(q):
        rows = pl.ds(q * 2 * LANE, 2 * LANE)
        for j in range(8):
            value = delay_ref[slab, rows, j * LANE : (j + 1) * LANE].astype(jnp.float32)
            wide[j, rows, :] = jnp.minimum(value, caps_ref[level, j // 4, 0:1, :])

    half_body(times_of(t_ref, 1 - parity()), convert, wide, out_ref, *scratch)


def kept_kernel(t_ref, wide, out_ref, *scratch):
    half_body(times_of(t_ref, parity()), lambda q: None, wide, out_ref, *scratch)


def half_max(level, caps, times, source, shape):
    levels, rows, width = shape
    work = HALF * SUB * rows * width
    vmem = pl.BlockSpec(memory_space=pltpu.VMEM)
    out = jax.ShapeDtypeStruct((HALF, 4, 2, SUB, LANE), jnp.float32)
    wide = jax.ShapeDtypeStruct((width // LANE, rows, LANE), jnp.float32)
    spread = pltpu.VMEM((TILES * SHIFT, HALF, SUB, LANE), jnp.float32)
    sent = level is not None
    return pl.pallas_call(
        functools.partial(sent_kernel, level) if sent else kept_kernel,
        out_shape=(out, wide) if sent else out,
        in_specs=[vmem] * (3 if sent else 2),
        out_specs=(vmem, vmem) if sent else vmem,
        scratch_shapes=[
            spread,
            spread,
            pltpu.VMEM((LANE // (SHIFT * TURNS), TILES, HALF, SUB, LANE), jnp.float32),
        ],
        compiler_params=pltpu.CompilerParams(vmem_limit_bytes=16 * 1024 * 1024),
        cost_estimate=pl.CostEstimate(flops=2 * work, bytes_accessed=2 * rows * width, transcendentals=0),
        name="sent_half" if sent else "kept_half",
    )(*((caps, times, source) if sent else (times, source)))


def exchange(value, axes):
    return lax.all_to_all(value, axes, split_axis=0, concat_axis=0, tiled=True)


def shards(arrival, delay, occupancy):
    scenarios, pins = arrival.shape
    levels = delay.shape[0]
    plane = lax.axis_size("x") * lax.axis_size("y")
    depth = lax.axis_size("z")
    place = lax.axis_index("x") * lax.axis_size("y") + lax.axis_index("y")
    odd = lax.axis_index("z") % 2
    col = lax.axis_index("z") * lax.axis_size("k") + lax.axis_index("k")
    flags = lax.dynamic_slice(occupancy, (0, col, place * 2), (levels, 1, 2))[:, 0, :]
    caps = jnp.where(flags > 0, jnp.float32(BOUND), jnp.float32(EMPTY))
    caps = jnp.broadcast_to(caps[:, :, None, None], (levels, 2, SUB, LANE))
    groups, tiles = scenarios // SUB, pins // LANE
    neighbour = [(z, z ^ 1) for z in range(depth)]
    times = jnp.transpose(arrival.reshape(groups, SUB, tiles, LANE), (0, 2, 1, 3))
    worst = None
    for level in range(levels):
        last = level == levels - 1
        sent, wide = half_max(level, caps, times, delay[:1] if level == 0 else delay, delay.shape)
        got = lax.ppermute(sent, "z", neighbour)
        kept = half_max(None, None, times, wide, delay.shape)
        best = jnp.maximum(kept, got)
        parts = best.reshape(plane * 2, 1, SUB, LANE)
        if last:
            top = jnp.max(jnp.max(best, axis=(1, 2)), axis=2)
            spot = lax.broadcasted_iota(jnp.int32, (HALF, SUB, LANE), 0) + odd * HALF
            here = lax.broadcasted_iota(jnp.int32, (HALF, SUB, LANE), 2) == spot
            top = jnp.max(jnp.where(here, top[:, :, None], EMPTY), axis=0)
            parts = jnp.concatenate([parts, jnp.broadcast_to(top[None, None], parts.shape)], axis=1)
        got = exchange(parts, ("x", "y", "k"))
        got = got.reshape(plane, 2, *got.shape[1:])
        got = jnp.maximum(got[:, 0], got[:, 1])
        if last:
            top = jnp.max(got[:, 1], axis=0)
            got = jnp.concatenate([got[:, :1], jnp.broadcast_to(top[None, None], (plane, 1, SUB, LANE))], axis=1)
        got = exchange(got, "z")
        if last:
            worst = jnp.transpose(jnp.max(got[:, 1], axis=0)[:, :groups]).reshape(scenarios)
        got = jnp.max(got[:, 0].reshape(depth // 2, 2, SUB, LANE), axis=0)
        whole = exchange(jnp.broadcast_to(got[None], (plane, 2, SUB, LANE)), ("x", "y"))
        times = whole.reshape(HALF, tiles, 2, SUB, LANE)
    final = jnp.transpose(times, (2, 0, 3, 1, 4)).reshape(scenarios, pins)
    return (final, worst)


def solution(mesh):
    shape = (4, 4, mesh.shape["col"] // 2, 2)
    fine = Mesh(np.asarray(mesh.devices).reshape(shape), ("x", "y", "z", "k"))
    col = ("z", "k")
    placed = (P(None, col), P(None, col, ("x", "y")), P())
    return jax.shard_map(
        shards, mesh=fine, in_specs=placed, out_specs=(P(None, col), P()), check_vma=False
    )
```

```python
import functools

import jax
import jax.numpy as jnp
import numpy as np
from jax import lax
from jax.experimental import pallas as pl
from jax.experimental.pallas import tpu as pltpu
from jax.sharding import Mesh
from jax.sharding import PartitionSpec as P

SUB, LANE = 8, 128
EMPTY = -1000000000.0
BOUND = 1000000000.0
HALF = 4
TILES = 4
SHIFT = 8
TURNS = 4


def half_body(times, convert, wide, out_ref, spread_a, spread_b, turned):
    rotations = LANE // (SHIFT * TURNS)
    chunk = TILES * SHIFT

    for m in range(rotations):
        for tile in range(TILES):
            for g in range(HALF):
                value = times(g, tile)
                turned[m, tile, g] = pltpu.roll(value, LANE - m * SHIFT * TURNS, 1) if m else value
    out_ref[...] = jnp.full(out_ref.shape, EMPTY, jnp.float32)

    def held_rows(m, q):
        return {(t, g): turned[m, q * 2 + t, g] for t in range(2) for g in range(HALF)}

    def spread_one(dest, e, q, place, held):
        a, t, g = place
        lane = e * SHIFT + a
        row = (q * 2 + t) * SHIFT + a
        dest[row, g] = jnp.broadcast_to(held[t, g][:, lane : lane + 1], (SUB, LANE))

    places = [(a, t, g) for a in range(SHIFT) for t in range(2) for g in range(HALF)]

    def warm(q, _):
        held = held_rows(0, q)
        for place in places:
            spread_one(spread_a, 0, q, place, held)
        convert(q)
        return 0

    for q in range(2):
        warm(q, 0)

    def stage(m, e, source, dest):
        next_m = m if e + 1 < TURNS else jnp.minimum(m + 1, rotations - 1)
        next_e = (e + 1) % TURNS

        def body(q, _):
            side = lax.rem(q, 2)
            late = (q // 2) * HALF
            held = held_rows(next_m, q)
            keys = [(g, j) for g in range(HALF) for j in range(4)]
            best = {(g, j): out_ref[g, j, side] for g, j in keys}
            todo = list(places)
            for k in range(chunk):
                place = (k // SHIFT) * LANE + e * SHIFT + k % SHIFT
                at = pl.ds(m * (SHIFT * TURNS) + place, 1)
                row = [jnp.broadcast_to(wide[side * 4 + j, at, :], (SUB, LANE)) for j in range(4)]
                for g in range(HALF):
                    value = source[k, late + g]
                    for j in range(4):
                        best[g, j] = jnp.maximum(best[g, j], value + row[j])
                for _ in range(2):
                    spread_one(dest, next_e, q, todo.pop(0), held)
            for g, j in keys:
                out_ref[g, j, side] = best[g, j]
            return 0

        lax.fori_loop(0, 2, body, 0)

    def rotation(m, _):
        for e in range(TURNS):
            pair = (spread_a, spread_b) if e % 2 == 0 else (spread_b, spread_a)
            stage(m, e, *pair)
        return 0

    lax.fori_loop(0, rotations, rotation, 0)


def times_of(t_ref, half):
    if len(t_ref.shape) == 4:
        return lambda g, tile: t_ref[half * HALF + g, tile]
    return lambda g, tile: t_ref[g, tile, half]


def parity():
    return lax.rem(lax.axis_index("z"), 2)


def sent_kernel(level, caps_ref, t_ref, delay_ref, out_ref, wide, *scratch):
    slab = level if delay_ref.shape[0] > 1 else 0

    def convert(q):
        rows = pl.ds(q * 2 * LANE, 2 * LANE)
        for j in range(8):
            value = delay_ref[slab, rows, j * LANE : (j + 1) * LANE].astype(jnp.float32)
            wide[j, rows, :] = jnp.minimum(value, caps_ref[level, j // 4, 0:1, :])

    half_body(times_of(t_ref, 1 - parity()), convert, wide, out_ref, *scratch)


def kept_kernel(t_ref, wide, out_ref, *scratch):
    half_body(times_of(t_ref, parity()), lambda q: None, wide, out_ref, *scratch)


def half_max(level, caps, times, source, shape):
    levels, rows, width = shape
    work = HALF * SUB * rows * width
    vmem = pl.BlockSpec(memory_space=pltpu.VMEM)
    out = jax.ShapeDtypeStruct((HALF, 4, 2, SUB, LANE), jnp.float32)
    wide = jax.ShapeDtypeStruct((width // LANE, rows, LANE), jnp.float32)
    spread = pltpu.VMEM((TILES * SHIFT, HALF, SUB, LANE), jnp.float32)
    sent = level is not None
    return pl.pallas_call(
        functools.partial(sent_kernel, level) if sent else kept_kernel,
        out_shape=(out, wide) if sent else out,
        in_specs=[vmem] * (3 if sent else 2),
        out_specs=(vmem, vmem) if sent else vmem,
        scratch_shapes=[
            spread,
            spread,
            pltpu.VMEM((LANE // (SHIFT * TURNS), TILES, HALF, SUB, LANE), jnp.float32),
        ],
        compiler_params=pltpu.CompilerParams(vmem_limit_bytes=16 * 1024 * 1024),
        cost_estimate=pl.CostEstimate(flops=2 * work, bytes_accessed=2 * rows * width, transcendentals=0),
        name="sent_half" if sent else "kept_half",
    )(*((caps, times, source) if sent else (times, source)))


def exchange(value, axes):
    return lax.all_to_all(value, axes, split_axis=0, concat_axis=0, tiled=True)


def shards(arrival, delay, occupancy):
    scenarios, pins = arrival.shape
    levels = delay.shape[0]
    plane = lax.axis_size("x") * lax.axis_size("y")
    depth = lax.axis_size("z")
    place = lax.axis_index("x") * lax.axis_size("y") + lax.axis_index("y")
    odd = lax.axis_index("z") % 2
    col = lax.axis_index("z") * lax.axis_size("k") + lax.axis_index("k")
    flags = lax.dynamic_slice(occupancy, (0, col, place * 2), (levels, 1, 2))[:, 0, :]
    caps = jnp.where(flags > 0, jnp.float32(BOUND), jnp.float32(EMPTY))
    caps = jnp.broadcast_to(caps[:, :, None, None], (levels, 2, SUB, LANE))
    groups, tiles = scenarios // SUB, pins // LANE
    neighbour = [(z, z ^ 1) for z in range(depth)]
    times = jnp.transpose(arrival.reshape(groups, SUB, tiles, LANE), (0, 2, 1, 3))
    worst = None
    for level in range(levels):
        last = level == levels - 1
        sent, wide = half_max(level, caps, times, delay[:1] if level == 0 else delay, delay.shape)
        got = lax.ppermute(sent, "z", neighbour)
        kept = half_max(None, None, times, wide, delay.shape)
        best = jnp.maximum(kept, got)
        parts = best.reshape(plane * 2, 1, SUB, LANE)
        if last:
            top = jnp.max(jnp.max(best, axis=(1, 2)), axis=2)
            spot = lax.broadcasted_iota(jnp.int32, (HALF, SUB, LANE), 0) + odd * HALF
            spot = spot * SUB + lax.broadcasted_iota(jnp.int32, (HALF, SUB, LANE), 1)
            here = lax.broadcasted_iota(jnp.int32, (HALF, SUB, LANE), 2) == spot
            top = jnp.max(jnp.where(here, top[:, :, None], EMPTY), axis=0)
            parts = jnp.concatenate([parts, jnp.broadcast_to(top[None, None], parts.shape)], axis=1)
        got = exchange(parts, ("x", "y", "k"))
        got = got.reshape(plane, 2, *got.shape[1:])
        got = jnp.maximum(got[:, 0], got[:, 1])
        if last:
            top = jnp.max(got[:, 1], axis=0)
            got = jnp.concatenate([got[:, :1], jnp.broadcast_to(top[None, None], (plane, 1, SUB, LANE))], axis=1)
        got = exchange(got, "z")
        if last:
            worst = jnp.max(got[:, 1], axis=(0, 1))[:scenarios]
        got = jnp.max(got[:, 0].reshape(depth // 2, 2, SUB, LANE), axis=0)
        if last:
            got, worst = lax.optimization_barrier((got, worst))
        whole = exchange(jnp.broadcast_to(got[None], (plane, 2, SUB, LANE)), ("x", "y"))
        times = whole.reshape(HALF, tiles, 2, SUB, LANE)
    final = jnp.transpose(times, (2, 0, 3, 1, 4)).reshape(scenarios, pins)
    return (final, worst)


def solution(mesh):
    shape = (4, 4, mesh.shape["col"] // 2, 2)
    fine = Mesh(np.asarray(mesh.devices).reshape(shape), ("x", "y", "z", "k"))
    col = ("z", "k")
    placed = (P(None, col), P(None, col, ("x", "y")), P())
    return jax.shard_map(
        shards, mesh=fine, in_specs=placed, out_specs=(P(None, col), P()), check_vma=False
    )
```

```python
import functools

import jax
import jax.numpy as jnp
import numpy as np
from jax import lax
from jax.experimental import pallas as pl
from jax.experimental.pallas import tpu as pltpu
from jax.sharding import Mesh
from jax.sharding import PartitionSpec as P

SUB, LANE = 8, 128
EMPTY = -1000000000.0
BOUND = 1000000000.0
HALF = 4
TILES = 4
SHIFT = 8
TURNS = 8
ROTATIONS = LANE // (SHIFT * TURNS)


def spread_one(dest, e, q, place, held):
    a, t, g = place
    lane = e * SHIFT + a
    row = (q * 2 + t) * SHIFT + a
    dest[row, g] = jnp.broadcast_to(held[t, g][:, lane : lane + 1], (SUB, LANE))


PLACES = [(a, t, g) for a in range(SHIFT) for t in range(2) for g in range(HALF)]


def held_rows(turned, m, q):
    return {(t, g): turned[m, q * 2 + t, g] for t in range(2) for g in range(HALF)}


def fill_turned(times, turned):
    for m in range(ROTATIONS):
        for tile in range(TILES):
            for g in range(HALF):
                value = times(g, tile)
                turned[m, tile, g] = pltpu.roll(value, LANE - m * SHIFT * TURNS, 1) if m else value


def half_loop(wide, out_ref, spread_a, spread_b, turned):
    chunk = TILES * SHIFT
    final = turned.shape[0] - 1

    def stage(m, e, source, dest):
        next_m = m if e + 1 < TURNS else jnp.minimum(m + 1, final)
        next_e = (e + 1) % TURNS

        def body(q, _):
            side = lax.rem(q, 2)
            late = (q // 2) * HALF
            held = held_rows(turned, next_m, q)
            keys = [(g, j) for g in range(HALF) for j in range(4)]
            best = {(g, j): out_ref[g, j, side] for g, j in keys}
            todo = list(PLACES)
            for k in range(chunk):
                place = (k // SHIFT) * LANE + e * SHIFT + k % SHIFT
                at = pl.ds(m * (SHIFT * TURNS) + place, 1)
                row = [jnp.broadcast_to(wide[side * 4 + j, at, :], (SUB, LANE)) for j in range(4)]
                for g in range(HALF):
                    value = source[k, late + g]
                    for j in range(4):
                        best[g, j] = jnp.maximum(best[g, j], value + row[j])
                for _ in range(2):
                    spread_one(dest, next_e, q, todo.pop(0), held)
            for g, j in keys:
                out_ref[g, j, side] = best[g, j]
            return 0

        lax.fori_loop(0, 2, body, 0)

    def rotation(m, _):
        for e in range(TURNS):
            pair = (spread_a, spread_b) if e % 2 == 0 else (spread_b, spread_a)
            stage(m, e, *pair)
        return 0

    lax.fori_loop(0, ROTATIONS, rotation, 0)


def times_of(t_ref, half):
    if len(t_ref.shape) == 4:
        return lambda g, tile: t_ref[half * HALF + g, tile]
    return lambda g, tile: t_ref[g, tile, half]


def sent_kernel(level, caps_ref, t_ref, delay_ref, out_ref, wide, kept_turned, kept_first, spread_b, turned):
    slab = level if delay_ref.shape[0] > 1 else 0
    odd = lax.rem(lax.axis_index("z"), 2)
    fill_turned(times_of(t_ref, 1 - odd), turned)
    fill_turned(times_of(t_ref, odd), kept_turned)
    for tile in range(TILES):
        for g in range(HALF):
            turned[ROTATIONS, tile, g] = times_of(t_ref, odd)(g, tile)
    out_ref[...] = jnp.full(out_ref.shape, EMPTY, jnp.float32)
    for q in range(2):
        held = held_rows(turned, 0, q)
        for place in PLACES:
            spread_one(kept_first, 0, q, place, held)
        rows = pl.ds(q * 2 * LANE, 2 * LANE)
        for j in range(8):
            value = delay_ref[slab, rows, j * LANE : (j + 1) * LANE].astype(jnp.float32)
            wide[j, rows, :] = jnp.minimum(value, caps_ref[level, j // 4, 0:1, :])
    half_loop(wide, out_ref, kept_first, spread_b, turned)


def kept_kernel(wide, turned, first, out_ref, spread_a, spread_b):
    out_ref[...] = jnp.full(out_ref.shape, EMPTY, jnp.float32)
    spread_a[...] = first[...]
    half_loop(wide, out_ref, spread_a, spread_b, turned)


def half_max(level, operands, shape):
    levels, rows, width = shape
    work = HALF * SUB * rows * width
    vmem = pl.BlockSpec(memory_space=pltpu.VMEM)
    out = jax.ShapeDtypeStruct((HALF, 4, 2, SUB, LANE), jnp.float32)
    wide = jax.ShapeDtypeStruct((width // LANE, rows, LANE), jnp.float32)
    tall, wider = (ROTATIONS, TILES, HALF, SUB, LANE), (ROTATIONS + 1, TILES, HALF, SUB, LANE)
    spread = (TILES * SHIFT, HALF, SUB, LANE)
    sent = level is not None
    outs = (out, wide, jax.ShapeDtypeStruct(tall, jnp.float32), jax.ShapeDtypeStruct(spread, jnp.float32))
    return pl.pallas_call(
        functools.partial(sent_kernel, level) if sent else kept_kernel,
        out_shape=outs if sent else out,
        in_specs=[vmem] * 3,
        out_specs=(vmem,) * 4 if sent else vmem,
        scratch_shapes=[pltpu.VMEM(spread, jnp.float32), pltpu.VMEM(wider if sent else spread, jnp.float32)],
        compiler_params=pltpu.CompilerParams(vmem_limit_bytes=16 * 1024 * 1024),
        cost_estimate=pl.CostEstimate(flops=2 * work, bytes_accessed=2 * rows * width, transcendentals=0),
        name="sent_half" if sent else "kept_half",
    )(*operands)


def exchange(value, axes):
    return lax.all_to_all(value, axes, split_axis=0, concat_axis=0, tiled=True)


def shards(arrival, delay, occupancy):
    scenarios, pins = arrival.shape
    levels = delay.shape[0]
    plane = lax.axis_size("x") * lax.axis_size("y")
    depth = lax.axis_size("z")
    place = lax.axis_index("x") * lax.axis_size("y") + lax.axis_index("y")
    odd = lax.axis_index("z") % 2
    col = lax.axis_index("z") * lax.axis_size("k") + lax.axis_index("k")
    flags = lax.dynamic_slice(occupancy, (0, col, place * 2), (levels, 1, 2))[:, 0, :]
    caps = jnp.where(flags > 0, jnp.float32(BOUND), jnp.float32(EMPTY))
    caps = jnp.broadcast_to(caps[:, :, None, None], (levels, 2, SUB, LANE))
    groups, tiles = scenarios // SUB, pins // LANE
    neighbour = [(z, z ^ 1) for z in range(depth)]
    times = jnp.transpose(arrival.reshape(groups, SUB, tiles, LANE), (0, 2, 1, 3))
    worst = None
    for level in range(levels):
        last = level == levels - 1
        source = delay[:1] if level == 0 else delay
        sent, *shared = half_max(level, (caps, times, source), delay.shape)
        got = lax.ppermute(sent, "z", neighbour)
        kept = half_max(None, shared, delay.shape)
        best = jnp.maximum(kept, got)
        parts = best.reshape(plane * 2, 1, SUB, LANE)
        if last:
            top = jnp.max(jnp.max(best, axis=(1, 2)), axis=2)
            spot = lax.broadcasted_iota(jnp.int32, (HALF, SUB, LANE), 0) + odd * HALF
            spot = spot * SUB + lax.broadcasted_iota(jnp.int32, (HALF, SUB, LANE), 1)
            here = lax.broadcasted_iota(jnp.int32, (HALF, SUB, LANE), 2) == spot
            top = jnp.max(jnp.where(here, top[:, :, None], EMPTY), axis=0)
            parts = jnp.concatenate([parts, jnp.broadcast_to(top[None, None], parts.shape)], axis=1)
        got = exchange(parts, ("x", "y", "k"))
        got = got.reshape(plane, 2, *got.shape[1:])
        got = jnp.maximum(got[:, 0], got[:, 1])
        if last:
            top = jnp.max(got[:, 1], axis=0)
            got = jnp.concatenate([got[:, :1], jnp.broadcast_to(top[None, None], (plane, 1, SUB, LANE))], axis=1)
        got = exchange(got, "z")
        if last:
            worst = jnp.max(got[:, 1], axis=(0, 1))[:scenarios]
        got = jnp.max(got[:, 0].reshape(depth // 2, 2, SUB, LANE), axis=0)
        if last:
            got, worst = lax.optimization_barrier((got, worst))
        whole = exchange(jnp.broadcast_to(got[None], (plane, 2, SUB, LANE)), ("x", "y"))
        times = whole.reshape(HALF, tiles, 2, SUB, LANE)
    final = jnp.transpose(times, (2, 0, 3, 1, 4)).reshape(scenarios, pins)
    return (final, worst)


def solution(mesh):
    shape = (4, 4, mesh.shape["col"] // 2, 2)
    fine = Mesh(np.asarray(mesh.devices).reshape(shape), ("x", "y", "z", "k"))
    col = ("z", "k")
    placed = (P(None, col), P(None, col, ("x", "y")), P())
    return jax.shard_map(
        shards, mesh=fine, in_specs=placed, out_specs=(P(None, col), P()), check_vma=False
    )
```

```python
import functools

import jax
import jax.numpy as jnp
import numpy as np
from jax import lax
from jax.experimental import pallas as pl
from jax.experimental.pallas import tpu as pltpu
from jax.sharding import Mesh
from jax.sharding import PartitionSpec as P

SUB, LANE = 8, 128
EMPTY = -1000000000.0
BOUND = 1000000000.0
HALF = 4
TILES = 4
SHIFT = 8
TURNS = 8
ROTATIONS = LANE // (SHIFT * TURNS)


def spread_one(dest, e, q, place, held):
    a, t, g = place
    lane = e * SHIFT + a
    row = (q * 2 + t) * SHIFT + a
    dest[row, g] = jnp.broadcast_to(held[t, g][:, lane : lane + 1], (SUB, LANE))


PLACES = [(a, t, g) for a in range(SHIFT) for t in range(2) for g in range(HALF)]


def held_rows(turned, m, q):
    return {(t, g): turned[m, q * 2 + t, g] for t in range(2) for g in range(HALF)}


def fill_turned(times, turned):
    for m in range(ROTATIONS):
        for tile in range(TILES):
            for g in range(HALF):
                value = times(g, tile)
                turned[m, tile, g] = pltpu.roll(value, LANE - m * SHIFT * TURNS, 1) if m else value


def half_loop(wide, out_ref, spread_a, spread_b, turned):
    chunk = TILES * SHIFT
    final = turned.shape[0] - 1

    def stage(m, e, source, dest):
        next_m = m if e + 1 < TURNS else jnp.minimum(m + 1, final)
        next_e = (e + 1) % TURNS

        def body(q, _):
            side = lax.rem(q, 2)
            late = (q // 2) * HALF
            held = held_rows(turned, next_m, q)
            keys = [(g, j) for g in range(HALF) for j in range(4)]
            best = {(g, j): out_ref[g, j, side] for g, j in keys}
            todo = list(PLACES)
            for k in range(chunk):
                place = (k // SHIFT) * LANE + e * SHIFT + k % SHIFT
                at = pl.ds(m * (SHIFT * TURNS) + place, 1)
                row = [jnp.broadcast_to(wide[side * 4 + j, at, :], (SUB, LANE)) for j in range(4)]
                for g in range(HALF):
                    value = source[k, late + g]
                    for j in range(4):
                        best[g, j] = jnp.maximum(best[g, j], value + row[j])
                for _ in range(2):
                    spread_one(dest, next_e, q, todo.pop(0), held)
            for g, j in keys:
                out_ref[g, j, side] = best[g, j]
            return 0

        lax.fori_loop(0, 2, body, 0)

    def rotation(m, _):
        for e in range(TURNS):
            pair = (spread_a, spread_b) if e % 2 == 0 else (spread_b, spread_a)
            stage(m, e, *pair)
        return 0

    lax.fori_loop(0, ROTATIONS, rotation, 0)


def times_of(t_ref, half):
    if len(t_ref.shape) == 4:
        return lambda g, tile: t_ref[half * HALF + g, tile]
    return lambda g, tile: t_ref[g, tile, half]


def first_kernel(occupancy_ref, t_ref, delay_ref, out_ref, wide, kept_turned, kept_first, caps_ref, *scratch):
    place = lax.axis_index("x") * lax.axis_size("y") + lax.axis_index("y")
    col = lax.axis_index("z") * lax.axis_size("k") + lax.axis_index("k")
    levels, _, width = occupancy_ref.shape
    lane = lax.broadcasted_iota(jnp.int32, (1, width), 1)
    for level in range(levels):
        row = occupancy_ref[level, pl.ds(col, 1), :].astype(jnp.float32)
        for side in range(2):
            flag = jnp.max(jnp.where(lane == place * 2 + side, row, 0.0), axis=1, keepdims=True)
            cap = jnp.where(flag > 0.0, jnp.float32(BOUND), jnp.float32(EMPTY))
            caps_ref[level, side] = jnp.broadcast_to(cap, (SUB, LANE))
    sent_kernel(0, caps_ref, t_ref, delay_ref, out_ref, wide, kept_turned, kept_first, *scratch)


def sent_kernel(level, caps_ref, t_ref, delay_ref, out_ref, wide, kept_turned, kept_first, spread_b, turned):
    slab = level if delay_ref.shape[0] > 1 else 0
    odd = lax.rem(lax.axis_index("z"), 2)
    fill_turned(times_of(t_ref, 1 - odd), turned)
    fill_turned(times_of(t_ref, odd), kept_turned)
    for tile in range(TILES):
        for g in range(HALF):
            turned[ROTATIONS, tile, g] = times_of(t_ref, odd)(g, tile)
    out_ref[...] = jnp.full(out_ref.shape, EMPTY, jnp.float32)
    for q in range(2):
        held = held_rows(turned, 0, q)
        for place in PLACES:
            spread_one(kept_first, 0, q, place, held)
        rows = pl.ds(q * 2 * LANE, 2 * LANE)
        for j in range(8):
            value = delay_ref[slab, rows, j * LANE : (j + 1) * LANE].astype(jnp.float32)
            wide[j, rows, :] = jnp.minimum(value, caps_ref[level, j // 4, 0:1, :])
    half_loop(wide, out_ref, kept_first, spread_b, turned)


def kept_kernel(wide, turned, first, out_ref, spread_a, spread_b):
    out_ref[...] = jnp.full(out_ref.shape, EMPTY, jnp.float32)
    spread_a[...] = first[...]
    half_loop(wide, out_ref, spread_a, spread_b, turned)


def half_max(level, operands, shape):
    levels, rows, width = shape
    work = HALF * SUB * rows * width
    vmem = pl.BlockSpec(memory_space=pltpu.VMEM)
    out = jax.ShapeDtypeStruct((HALF, 4, 2, SUB, LANE), jnp.float32)
    wide = jax.ShapeDtypeStruct((width // LANE, rows, LANE), jnp.float32)
    tall, wider = (ROTATIONS, TILES, HALF, SUB, LANE), (ROTATIONS + 1, TILES, HALF, SUB, LANE)
    spread = (TILES * SHIFT, HALF, SUB, LANE)
    sent = level is not None
    outs = (out, wide, jax.ShapeDtypeStruct(tall, jnp.float32), jax.ShapeDtypeStruct(spread, jnp.float32))
    kernel = functools.partial(sent_kernel, level) if sent else kept_kernel
    if level == 0:
        kernel = first_kernel
        outs += (jax.ShapeDtypeStruct((levels, 2, SUB, LANE), jnp.float32),)
    return pl.pallas_call(
        kernel,
        out_shape=outs if sent else out,
        in_specs=[vmem] * 3,
        out_specs=(vmem,) * len(outs) if sent else vmem,
        scratch_shapes=[pltpu.VMEM(spread, jnp.float32), pltpu.VMEM(wider if sent else spread, jnp.float32)],
        compiler_params=pltpu.CompilerParams(vmem_limit_bytes=16 * 1024 * 1024),
        cost_estimate=pl.CostEstimate(flops=2 * work, bytes_accessed=2 * rows * width, transcendentals=0),
        name="sent_half" if sent else "kept_half",
    )(*operands)


def exchange(value, axes):
    return lax.all_to_all(value, axes, split_axis=0, concat_axis=0, tiled=True)


def shards(arrival, delay, occupancy):
    scenarios, pins = arrival.shape
    levels = delay.shape[0]
    plane = lax.axis_size("x") * lax.axis_size("y")
    depth = lax.axis_size("z")
    odd = lax.axis_index("z") % 2
    caps = occupancy
    groups, tiles = scenarios // SUB, pins // LANE
    neighbour = [(z, z ^ 1) for z in range(depth)]
    times = jnp.transpose(arrival.reshape(groups, SUB, tiles, LANE), (0, 2, 1, 3))
    worst = None
    for level in range(levels):
        last = level == levels - 1
        source = delay[:1] if level == 0 else delay
        sent, *shared = half_max(level, (caps, times, source), delay.shape)
        if level == 0:
            caps = shared.pop()
        got = lax.ppermute(sent, "z", neighbour)
        kept = half_max(None, shared, delay.shape)
        best = jnp.maximum(kept, got)
        parts = best.reshape(plane * 2, 1, SUB, LANE)
        if last:
            top = jnp.max(jnp.max(best, axis=(1, 2)), axis=2)
            spot = lax.broadcasted_iota(jnp.int32, (HALF, SUB, LANE), 0) + odd * HALF
            spot = spot * SUB + lax.broadcasted_iota(jnp.int32, (HALF, SUB, LANE), 1)
            here = lax.broadcasted_iota(jnp.int32, (HALF, SUB, LANE), 2) == spot
            top = jnp.max(jnp.where(here, top[:, :, None], EMPTY), axis=0)
            parts = jnp.concatenate([parts, jnp.broadcast_to(top[None, None], parts.shape)], axis=1)
        got = exchange(parts, ("x", "y", "k"))
        got = got.reshape(plane, 2, *got.shape[1:])
        got = jnp.maximum(got[:, 0], got[:, 1])
        if last:
            top = jnp.max(got[:, 1], axis=0)
            got = jnp.concatenate([got[:, :1], jnp.broadcast_to(top[None, None], (plane, 1, SUB, LANE))], axis=1)
        got = exchange(got, "z")
        if last:
            worst = jnp.max(got[:, 1], axis=(0, 1))[:scenarios]
        got = jnp.max(got[:, 0].reshape(depth // 2, 2, SUB, LANE), axis=0)
        if last:
            got, worst = lax.optimization_barrier((got, worst))
        whole = exchange(jnp.broadcast_to(got[None], (plane, 2, SUB, LANE)), ("x", "y"))
        times = whole.reshape(HALF, tiles, 2, SUB, LANE)
    final = jnp.transpose(times, (2, 0, 3, 1, 4)).reshape(scenarios, pins)
    return (final, worst)


def solution(mesh):
    shape = (4, 4, mesh.shape["col"] // 2, 2)
    fine = Mesh(np.asarray(mesh.devices).reshape(shape), ("x", "y", "z", "k"))
    col = ("z", "k")
    placed = (P(None, col), P(None, col, ("x", "y")), P())
    return jax.shard_map(
        shards, mesh=fine, in_specs=placed, out_specs=(P(None, col), P()), check_vma=False
    )
```
